512 devices in a mesh: gx: 8 (over x, z_lo), gy: 4 (over z_hi), gz: 16 (over y, core).
Axes of the slice: x: 4, y: 8, z: 8 (z_hi: 4, z_lo: 2; z = z_hi * 2 + z_lo), core: 2. Of those that a mesh axis runs over, the one named last changes fastest.
Arguments:
- density: float32 [768, 1024, 512], P('gz', 'gx', 'gy'), may hold values from 0.0005 to 0.01
- shear_offsets: int32 [2, 768], P(None, 'gz'), may hold values from 0 to 192, as said below
- shear_fractions: float32 [2, 768], P(None, 'gz'), may hold values from 0 to 1
- flat_field: float32 [1024, 512], P(('gx', 'gz'), 'gy'), may hold values from 0.5 to 1.5
Outputs:
- normalized: float32 [1024, 512], P(('gx', 'gz'), 'gy')
The draws below stay inside these ranges and needn't reach their ends.
Inputs may be any that keep to these rules, and one draw needn't show every extreme that they name: `shear_offsets`: in each row, the shift never falls from one slice to the next and rises by at most 1; it is 0 or 1 at slice 0 and exactly 192 at the last slice.
All inputs are finite; a program needn't handle non-finite values.
Results may differ from the reference program's by a relative error of at most 0.0003.
Values sent between devices are 32-bit elements; how exact they have to be, the bound alone decides.
A program may use at most 64 MiB of HBM per device.

```python
import math
import jax
import jax.numpy as jnp
from jax import lax

NX = 1024
NY = 512
NZ = 768


def draw_shear_offsets(key, part):
    rows_list = []
    for component in range(2):
        shuffled = jax.random.permutation(jax.random.fold_in(key, 11 + component), NZ)
        rising = (shuffled < NZ // 4).astype(jnp.int32)
        rows_list.append(jnp.cumsum(rising).astype(jnp.int32))
    return jnp.stack(rows_list, axis=0)


def steps_of(stream_key, extent, shards, least, high):
    def one(dim, parts):
        draws = jax.random.uniform(jax.random.fold_in(jax.random.fold_in(stream_key, 6), dim), (parts,), jnp.float32, least / len(shards), high / len(shards))
        return jnp.repeat(jnp.exp(draws), extent[dim] // parts).reshape((-1,) + (1,) * (len(extent) - dim - 1))

    level = one(*shards[0])
    for cut in shards[1:]:
        level = level * one(*cut)
    return level


def setup_inputs(seed: int = 0) -> dict:
    keys = jax.random.split(jax.random.key(seed), 5)
    density = jnp.clip(jnp.exp(math.log(0.01) - 2.9957322 * jax.random.uniform(keys[0], (NZ, NX, NY), jnp.float32) ** steps_of(keys[0], (NZ, NX, NY), ((0, 16), (1, 8), (2, 4)), -0.2, 0.2)), 0.0005, 0.01)
    shear_offsets = draw_shear_offsets(jax.random.fold_in(keys[4], 71), 0)
    shear_fractions = jnp.clip(1.0 * jax.random.uniform(keys[2], (2, NZ), jnp.float32) ** steps_of(keys[2], (2, NZ), ((1, 16),), -0.2, 0.2), 0.0, 1.0)
    flat_field = jnp.clip(1.0 + 0.1 * jax.random.normal(keys[3], (NX, NY), jnp.float32), 0.5, 1.5)
    return {"density": density, "shear_offsets": shear_offsets, "shear_fractions": shear_fractions, "flat_field": flat_field}


def splat_slab(screen, slab, start_u, start_v, frac_u, frac_v):
    height, width = slab.shape
    spread = jnp.pad(slab * ((1.0 - frac_u) * (1.0 - frac_v)), ((0, 1), (0, 1)))
    spread = spread + jnp.pad(slab * (frac_u * (1.0 - frac_v)), ((1, 0), (0, 1)))
    spread = spread + jnp.pad(slab * ((1.0 - frac_u) * frac_v), ((0, 1), (1, 0)))
    spread = spread + jnp.pad(slab * (frac_u * frac_v), ((1, 0), (1, 0)))
    window = lax.dynamic_slice(screen, (start_u, start_v), (height + 1, width + 1))
    return lax.dynamic_update_slice(screen, window + spread, (start_u, start_v))


def reference(density, shear_offsets, shear_fractions, flat_field):
    center = NZ // 8
    margin = center + 1
    screen = jnp.zeros((NX + 2 * margin, NY + 2 * margin), jnp.float32)

    def march_slab(carry, inputs):
        slab, offset_pair, frac_pair = inputs
        start_u = (offset_pair[0] - center + margin).astype(jnp.int32)
        start_v = (offset_pair[1] - center + margin).astype(jnp.int32)
        return splat_slab(carry, slab, start_u, start_v, frac_pair[0], frac_pair[1]), None

    screen, unused = lax.scan(march_slab, screen, (density, shear_offsets.T, shear_fractions.T))
    integral = screen[margin:margin + NX, margin:margin + NY]
    detected = flat_field * jnp.exp(-integral)
    return detected / jnp.max(detected)
```

```python
import functools

import jax
import jax.numpy as jnp
from jax import lax
from jax.experimental import pallas as pl
from jax.experimental.pallas import tpu as pltpu
from jax.sharding import PartitionSpec as P

MESH = pl.DeviceIdType.MESH
ROWS = 8
LANES = 128
CHUNKS = 4


def remote(src, dst, send_sem, recv_sem, device_id):
    return pltpu.make_async_remote_copy(
        src_ref=src, dst_ref=dst, send_sem=send_sem, recv_sem=recv_sem, device_id=device_id, device_id_type=MESH
    )


def march(bufs, offs, fracs, lane, chunk, accs):
    per = bufs[0].shape[0]
    base_u = offs[0, 0]
    base_v = offs[1, 0]
    pad = (bufs[0].shape[1] - LANES) // 2
    vregs = len(accs) // 2
    buf = bufs[chunk]

    def one(local, accs):
        z = chunk * per + local
        su = offs[0, z] - base_u
        sv = offs[1, z] - base_v
        fu = fracs[0, z]
        fv = fracs[1, z]
        gu = 1.0 - fu
        gv = 1.0 - fv
        early = lane < sv
        early1 = lane <= sv
        wa0 = jnp.where(early, 0.0, gv)
        wb0 = jnp.where(early, gv, 0.0)
        wa1 = jnp.where(early1, 0.0, fv)
        wb1 = jnp.where(early1, fv, 0.0)
        out = []
        for j in range(vregs):
            here = buf[local, pl.ds(ROWS * j + pad - su, ROWS), :]
            before = buf[local, pl.ds(ROWS * j + pad - 1 - su, ROWS), :]
            q = here * gu + before * fu
            r0 = pltpu.roll(q, sv, 1)
            r1 = pltpu.roll(r0, 1, 1)
            out.append(accs[2 * j] + (r0 * wa0 + r1 * wa1))
            out.append(accs[2 * j + 1] + (r0 * wb0 + r1 * wb1))
        return tuple(out)

    return lax.fori_loop(0, per, one, accs)


def kernel(
    sizes, offs, fracs, flat, density, out,
    buf0, buf1, buf2, buf3, win, frame, summed, got_pair, got_y, red, got_halo, peak, got_m1, peak2, got_m2,
    sem_in, s_pair, r_pair, s_y, r_y, s_halo, r_halo, s_m1, r_m1, s_m2, r_m2,
):
    nx, ny, nz = sizes
    chips = nz // 2
    bufs = (buf0, buf1, buf2, buf3)
    per = buf0.shape[0]
    pad = (buf0.shape[1] - LANES) // 2
    gx = lax.axis_index("gx")
    gy = lax.axis_index("gy")
    gz = lax.axis_index("gz")
    chip = gz // 2
    core = gz % 2
    plane = gx * ny + gy

    loads = [
        pltpu.make_async_copy(
            density.at[pl.ds(c * per, per)], bufs[c].at[:, pl.ds(pad, LANES), :], sem_in.at[c]
        )
        for c in range(CHUNKS)
    ]
    for load in loads:
        load.start()

    barrier = pltpu.get_barrier_semaphore()

    def greet_z(d, carry):
        pl.semaphore_signal(barrier, inc=1, device_id={"gz": (gz + d) % nz}, device_id_type=MESH)
        return carry

    def greet_plane(d, carry):
        other = (plane + d) % (nx * ny)
        pl.semaphore_signal(
            barrier, inc=1, device_id={"gx": other // ny, "gy": other % ny}, device_id_type=MESH
        )
        return carry

    lax.fori_loop(1, nz, greet_z, 0)
    lax.fori_loop(1, nx * ny, greet_plane, 0)

    zero = jnp.zeros((ROWS, LANES), jnp.float32)
    edge = jnp.zeros((pad, LANES), jnp.float32)
    for c in range(CHUNKS):
        for local in range(per):
            bufs[c][local, pl.ds(0, pad), :] = edge
            bufs[c][local, pl.ds(pad + LANES, pad), :] = edge
    vregs = (LANES + pad) // ROWS
    top = 192
    total = win.shape[1]
    for half in range(2):
        win[half, pl.ds(0, top), :] = jnp.zeros((top, LANES), jnp.float32)
        rest = total - top - vregs * ROWS
        win[half, pl.ds(top + vregs * ROWS, rest), :] = jnp.zeros((rest, LANES), jnp.float32)

    lane = lax.broadcasted_iota(jnp.int32, (ROWS, LANES), 1)
    accs = (zero,) * (2 * vregs)
    for c in range(CHUNKS):
        loads[c].wait()
        accs = march(bufs, offs, fracs, lane, c, accs)
    for j in range(vregs):
        for half in range(2):
            win[half, pl.ds(top + ROWS * j, ROWS), :] = accs[2 * j + half]

    blocks = LANES // ROWS
    base_u = offs[0, 0]
    shift = offs[1, 0] + 32
    wide = shift >= LANES
    turn = jnp.where(wide, shift - LANES, shift)
    first = lane < turn
    far = jnp.full((ROWS, LANES), shift, jnp.int32) >= LANES
    for j in range(3 * blocks):
        tu, rb = j // blocks, j % blocks
        if ROWS * j < 32 or ROWS * j > 32 + 192 + LANES:
            tiles = (zero, zero, zero)
        else:
            start = ROWS * j - 32 + top - base_u
            ra = pltpu.roll(win[0, pl.ds(start, ROWS), :], turn, 1)
            rb_ = pltpu.roll(win[1, pl.ds(start, ROWS), :], turn, 1)
            x0 = jnp.where(first, 0.0, ra)
            x1 = jnp.where(first, ra, rb_)
            x2 = jnp.where(first, rb_, 0.0)
            tiles = (jnp.where(far, 0.0, x0), jnp.where(far, x0, x1), jnp.where(far, x1, x2))
        for tv in range(3):
            frame[rb % 2, rb // 2, 3 * tu + tv] = tiles[tv]

    pl.semaphore_wait(barrier, nz - 1 + nx * ny - 1)

    swap = remote(frame.at[1 - core], got_pair, s_pair, r_pair, {"gz": chip * 2 + 1 - core})
    swap.start()
    swap.wait_recv()

    def y_copy(d):
        to = (chip + d) % chips
        return to, remote(
            summed.at[to], got_y.at[d], s_y.at[d], r_y.at[d], {"gz": to * 2 + core}
        )

    order = sorted(range(1, chips), key=lambda d: -min(d, chips - d))
    sends = []
    for d in order:
        to, copy = y_copy(d)
        summed[to] = frame[core, to] + got_pair[to]
        copy.start()
        sends.append(copy)
    mine = frame[core, chip] + got_pair[chip]
    for d in reversed(order):
        y_copy(d)[1].wait_recv()
        mine = mine + got_y[d]
    red[...] = mine

    steps = [(tu, tv) for tu in (0, 2) for tv in (0, 2)] + [(0, 1), (2, 1), (1, 0), (1, 2)]

    def inside(u, v):
        return (u >= 0) & (u < nx) & (v >= 0) & (v < ny)

    def halo(tu, tv):
        t = 3 * tu + tv
        return remote(
            red.at[t], got_halo.at[t], s_halo.at[t], r_halo.at[t], {"gx": gx + tu - 1, "gy": gy + tv - 1}
        )

    for tu, tv in steps:
        @pl.when(inside(gx + tu - 1, gy + tv - 1))
        def _():
            halo(tu, tv).start()

        @pl.when(jnp.logical_not(inside(gx - tu + 1, gy - tv + 1)))
        def _():
            got_halo[3 * tu + tv] = zero

    integral = mine[4]
    for tu, tv in reversed(steps):
        @pl.when(inside(gx - tu + 1, gy - tv + 1))
        def _():
            halo(tu, tv).wait_recv()

        integral = integral + got_halo[3 * tu + tv]

    detected = flat[...] * jnp.exp(-integral)
    top_row = jnp.max(detected, axis=0, keepdims=True)
    peak[0] = top_row

    def m1_copy(d):
        return remote(peak, got_m1.at[d], s_m1.at[d], r_m1.at[d], {"gz": (gz + d) % nz})

    def m2_copy(d):
        other = (plane + d) % (nx * ny)
        return remote(
            peak2, got_m2.at[d], s_m2.at[d], r_m2.at[d], {"gx": other // ny, "gy": other % ny}
        )

    def spread(copy_of, count):
        def go(d, carry):
            copy_of(d).start()
            return carry

        lax.fori_loop(1, count, go, 0)

    def collect(copy_of, got, count, largest):
        def take(d, largest):
            copy_of(d).wait_recv()
            return jnp.maximum(largest, got[d, 0])

        return lax.fori_loop(1, count, take, largest)

    spread(m1_copy, nz)
    largest = collect(m1_copy, got_m1, nz, top_row)
    peak2[0] = largest
    spread(m2_copy, nx * ny)
    largest = collect(m2_copy, got_m2, nx * ny, largest)
    out[...] = detected / jnp.max(largest)

    swap.wait_send()
    for copy in sends:
        copy.wait_send()
    for tu, tv in steps:
        @pl.when(inside(gx + tu - 1, gy + tv - 1))
        def _():
            halo(tu, tv).wait_send()

    def sent(copy_of, count):
        def done(d, carry):
            copy_of(d).wait_send()
            return carry

        lax.fori_loop(1, count, done, 0)

    sent(m1_copy, nz)
    sent(m2_copy, nx * ny)


def shards(sizes, density, shear_offsets, shear_fractions, flat_field):
    nx, ny, nz = sizes
    slices = density.shape[0]
    chips = nz // 2
    pad = slices
    vmem = pltpu.VMEM
    dma = pltpu.SemaphoreType.DMA
    f32 = jnp.float32
    smem = pl.BlockSpec(memory_space=pltpu.SMEM)
    invmem = pl.BlockSpec(memory_space=pltpu.VMEM)
    return pl.pallas_call(
        functools.partial(kernel, sizes),
        out_shape=jax.ShapeDtypeStruct(flat_field.shape, f32),
        in_specs=[smem, smem, invmem, pl.BlockSpec(memory_space=pl.ANY)],
        out_specs=invmem,
        scratch_shapes=[vmem((slices // CHUNKS, LANES + 2 * pad, LANES), f32) for _ in range(CHUNKS)]
        + [
            vmem((2, 528, LANES), f32),
            vmem((2, chips, 9, ROWS, LANES), f32),
            vmem((chips, 9, ROWS, LANES), f32),
            vmem((chips, 9, ROWS, LANES), f32),
            vmem((chips, 9, ROWS, LANES), f32),
            vmem((9, ROWS, LANES), f32),
            vmem((9, ROWS, LANES), f32),
            vmem((1, 1, LANES), f32),
            vmem((nz, 1, 1, LANES), f32),
            vmem((1, 1, LANES), f32),
            vmem((nx * ny, 1, 1, LANES), f32),
            dma((CHUNKS,)),
            dma, dma,
            dma((chips,)), dma((chips,)),
            dma((9,)), dma((9,)),
            dma((nz,)), dma((nz,)),
            dma((nx * ny,)), dma((nx * ny,)),
        ],
        compiler_params=pltpu.CompilerParams(collective_id=0, has_side_effects=True),
    )(shear_offsets, shear_fractions, flat_field, density)


def solution(mesh):
    sizes = (mesh.shape["gx"], mesh.shape["gy"], mesh.shape["gz"])
    return jax.shard_map(
        functools.partial(shards, sizes),
        mesh=mesh,
        in_specs=(P("gz", "gx", "gy"), P(None, "gz"), P(None, "gz"), P(("gx", "gz"), "gy")),
        out_specs=P(("gx", "gz"), "gy"),
        check_vma=False,
    )
```
